32 devices in a mesh: gx: 4 (over z), gy: 4 (over x, core), gz: 2 (over y).
Axes of the slice: x: 2, y: 2, z: 4, core: 2. Of those that a mesh axis runs over, the one named last changes fastest.
Arguments:
- pair: bfloat16 [1024, 1024, 128], P('gx', 'gy'), may hold values from -8 to 8, as said below
- residue_mask: int32 [1024], replicated, may hold values 0 or 1
- ln_in_gain: float32 [128], replicated, may hold values from 0.1 to 1.9
- w_proj: bfloat16 [128, 4, 128], P(None, None, 'gz'), may hold values from -0.5 to 0.5
- w_gate: bfloat16 [128, 128], replicated, may hold values from -0.5 to 0.5
- ln_out_gain: float32 [128], replicated, may hold values from 0.1 to 1.9
- w_out: bfloat16 [128, 128], replicated, may hold values from -0.5 to 0.5
Outputs:
- update: bfloat16 [128, 1024, 1024], P(None, ('gx', 'gz'), 'gy')
- energy: float32 [], replicated
The draws below stay inside these ranges and needn't reach their ends.
Inputs may be any that keep to these rules, and one draw needn't show every extreme that they name: pair is symmetric in its two residue indices: pair[i, j, c] equals pair[j, i, c].
All inputs are finite; a program needn't handle non-finite values.
Results may differ from the reference program's by a relative error of at most 0.0083.
Values may be sent and summed in bfloat16 or wider, within the bound.
A program may use at most 256 MiB of HBM per device.

```python
import math
import jax
import jax.numpy as jnp
from jax import lax

C = 128
H = 128
N = 1024


def draw_pair(key, part):
    base_key = jax.random.fold_in(key, 11)
    base_draw = jax.random.normal(base_key, (N, N, C), jnp.float32)
    symmetric = (base_draw + jnp.swapaxes(base_draw, 0, 1)) * 0.7071
    return jnp.clip(symmetric, -8.0, 8.0).astype(jnp.bfloat16)


def set_ends(array, stream_key, low, high):
    longest = array.shape.index(max(array.shape))
    spots = []
    for shift in (0, 1):
        where = [jax.random.randint(jax.random.fold_in(stream_key, axis), (), 0, length) for axis, length in enumerate(array.shape)]
        where[longest] = (where[longest] + shift) % array.shape[longest]
        spots.append(tuple(where))
    return array.at[spots[0]].set(low).at[spots[1]].set(high)


def block_scale(rng, shape, split, smallest, high):
    gain, own = 1.0, jax.random.fold_in(rng, 6)
    for axis_at, shards_of in split:
        heights = jnp.exp(jax.random.uniform(jax.random.fold_in(own, axis_at), (shards_of,), jnp.float32, smallest / len(split), high / len(split)))
        gain = gain * jnp.repeat(heights, shape[axis_at] // shards_of).reshape([-1 if axis == axis_at else 1 for axis in range(len(shape))])
    return gain


def bell_draw(stream_key, shape, width, most, pieces=(), held_as=jnp.bfloat16):
    entries = jax.random.normal(stream_key, shape, jnp.float32) * width
    if len(pieces) > 0:
        entries = block_scale(stream_key, shape, pieces, -0.22, 0.18) * entries
    return jnp.clip(entries, min=-most, max=most).astype(held_as)


def setup_inputs(seed: int = 0) -> dict:
    seeds = jax.random.split(jax.random.key(seed), 8)
    pair = draw_pair(jax.random.fold_in(seeds[7], 71), 0)
    residue_mask = set_ends((jax.random.randint(seeds[1], (N,), 0, 8) < 7).astype(jnp.int32), jax.random.fold_in(seeds[1], 1), 0, 1)
    ln_in_gain = jnp.clip(1.0 + 0.18 * jax.random.normal(seeds[2], (C,), jnp.float32), 0.1, 1.9)
    w_proj = bell_draw(seeds[3], (C, 4, H), C ** -0.5, 0.5, ((2, 2),))
    w_gate = bell_draw(seeds[4], (C, C), C ** -0.5, 0.5)
    ln_out_gain = jnp.clip(1.0 + 0.18 * jax.random.normal(seeds[5], (H,), jnp.float32), 0.1, 1.9)
    w_out = bell_draw(seeds[6], (H, C), H ** -0.5, 0.5)
    return dict(pair=pair, residue_mask=residue_mask, ln_in_gain=ln_in_gain, w_proj=w_proj, w_gate=w_gate, ln_out_gain=ln_out_gain, w_out=w_out)


NORM_EPS = 1e-05

def layer_norm(values, gain_vec, axis):
    mean_val = lax.optimization_barrier(jnp.mean(values, axis=axis, keepdims=True))
    centred = values - mean_val
    variance = lax.optimization_barrier(jnp.mean(centred * centred, axis=axis, keepdims=True))
    return centred * lax.rsqrt(variance + NORM_EPS) * gain_vec

def reference(pair, residue_mask, ln_in_gain, w_proj, w_gate, ln_out_gain, w_out):
    block_rows = math.gcd(N, 128)
    block_count = N // block_rows
    mask_float = residue_mask.astype(jnp.float32)
    normed = layer_norm(pair.astype(jnp.float32), ln_in_gain, -1).astype(jnp.bfloat16)
    normed_blocks = normed.reshape(block_count, block_rows, N, C)
    mask_blocks = mask_float.reshape(block_count, block_rows)

    def project(inputs):
        normed_block, mask_block = inputs
        projected = jnp.einsum('ijd,dkh->khij', normed_block.astype(jnp.float32), w_proj.astype(jnp.float32))
        masked = mask_block[:, None] * mask_float[None, :]
        left_block = (masked * jax.nn.sigmoid(projected[0]) * projected[1]).astype(jnp.bfloat16)
        right_block = (masked * jax.nn.sigmoid(projected[2]) * projected[3]).astype(jnp.bfloat16)
        return (left_block, right_block)
    left_all, right_all = lax.map(project, (normed_blocks, mask_blocks))
    left_all = jnp.transpose(left_all, (1, 0, 2, 3)).reshape(H, N, N)
    right_all = jnp.transpose(right_all, (1, 0, 2, 3)).reshape(H, N, N)

    def triangle(inputs):
        left_mat, right_mat = inputs
        product = jnp.dot(left_mat, right_mat, preferred_element_type=jnp.float32)
        product = product + jnp.dot(right_mat, left_mat, preferred_element_type=jnp.float32)
        return (0.5 * product).astype(jnp.bfloat16)
    tri_map = lax.map(triangle, (left_all, right_all))
    tri_blocks = jnp.transpose(tri_map.reshape(H, block_count, block_rows, N), (1, 0, 2, 3))

    def finish(inputs):
        tri_block, normed_block = inputs
        tri_normed = layer_norm(tri_block.astype(jnp.float32), ln_out_gain[:, None, None], 0).astype(jnp.bfloat16)
        gate_vals = jax.nn.sigmoid(jnp.einsum('ijd,dc->cij', normed_block.astype(jnp.float32), w_gate.astype(jnp.float32)))
        mixed = jnp.einsum('hij,hc->cij', tri_normed.astype(jnp.float32), w_out.astype(jnp.float32))
        return (gate_vals * mixed).astype(jnp.bfloat16)
    updated = lax.map(finish, (tri_blocks, normed_blocks))
    update = jnp.transpose(updated, (1, 0, 2, 3)).reshape(C, N, N)
    positions = jnp.arange(N, dtype=jnp.int32).astype(jnp.float32)
    weighting = (1.0 + (positions[:, None] + positions[None, :]) / N) * mask_float[:, None] * mask_float[None, :]
    squares = update.astype(jnp.float32) * update.astype(jnp.float32)
    energy = jnp.sum(squares * weighting[None]) / (N * N * C)
    return (update, energy)
```

```python
import jax
import jax.numpy as jnp
from jax import lax
from jax.sharding import PartitionSpec as P

NORM_EPS = 1e-05


def layer_norm(values, gain_vec, axis):
    mean_val = jnp.mean(values, axis=axis, keepdims=True)
    centred = values - mean_val
    variance = jnp.mean(centred * centred, axis=axis, keepdims=True)
    return centred * lax.rsqrt(variance + NORM_EPS) * gain_vec


def batched(first, second):
    return jnp.einsum("hik,hkj->hij", first, second, preferred_element_type=jnp.float32)


def local(pair, residue_mask, ln_in_gain, w_proj, w_gate, ln_out_gain, w_out):
    tile_len = pair.shape[0]
    channel_count = pair.shape[2]
    grid_len = lax.axis_size("gx")
    slab_count = lax.axis_size("gz")
    slab_rows = tile_len // slab_count
    total_len = tile_len * grid_len
    row_block = lax.axis_index("gx")
    col_block = lax.axis_index("gy")
    slab_index = lax.axis_index("gz")
    mask_float = residue_mask.astype(jnp.float32)
    row_mask = lax.dynamic_slice_in_dim(mask_float, row_block * tile_len, tile_len)
    col_mask = lax.dynamic_slice_in_dim(mask_float, col_block * tile_len, tile_len)
    tile_mask = row_mask[:, None] * col_mask[None, :]
    normed = layer_norm(pair.astype(jnp.float32), ln_in_gain, -1).astype(jnp.bfloat16)
    projected = jnp.einsum("ijd,dkh->khij", normed, w_proj, preferred_element_type=jnp.float32)
    left_tile = (tile_mask * jax.nn.sigmoid(projected[0]) * projected[1]).astype(jnp.bfloat16)
    right_tile = (tile_mask * jax.nn.sigmoid(projected[2]) * projected[3]).astype(jnp.bfloat16)
    col_len = pair.shape[1]
    col_count = lax.axis_size("gy")
    own_count = left_tile.shape[0] // (grid_len * col_count)

    def whole(tile):
        spread = lax.all_to_all(tile, ("gx", "gy"), split_axis=0, concat_axis=0, tiled=True)
        spread = spread.reshape(grid_len, col_count, own_count, tile_len, col_len)
        return spread.transpose(2, 0, 3, 1, 4).reshape(own_count, total_len, total_len)

    left = whole(left_tile)
    right = whole(right_tile)
    summed = batched(left, right) + batched(right, left)
    tri_map = (0.5 * summed).astype(jnp.bfloat16)
    outgoing = tri_map.reshape(own_count, grid_len, slab_count, slab_rows, col_count, col_len)
    outgoing = outgoing.transpose(1, 4, 2, 0, 3, 5).reshape(-1, slab_rows, col_len)
    arrived = lax.all_to_all(outgoing, ("gx", "gy", "gz"), split_axis=0, concat_axis=0, tiled=True)

    def by_arrival(table):
        parts = table.reshape((slab_count, grid_len, col_count, own_count) + table.shape[1:])
        return jnp.moveaxis(parts, 0, 2).reshape(table.shape)

    ln_out_gain = by_arrival(ln_out_gain)
    w_out = by_arrival(w_out)
    tri_normed = layer_norm(arrived.astype(jnp.float32), ln_out_gain[:, None, None], 0).astype(jnp.bfloat16)
    mixed = jnp.einsum("hij,hc->cij", tri_normed, w_out, preferred_element_type=jnp.float32)
    slab_normed = lax.dynamic_slice_in_dim(normed, slab_index * slab_rows, slab_rows, 0)
    gate_vals = jax.nn.sigmoid(
        jnp.einsum("ijd,dc->cij", slab_normed, w_gate, preferred_element_type=jnp.float32)
    )
    update = (gate_vals * mixed).astype(jnp.bfloat16)
    row_start = row_block * tile_len + slab_index * slab_rows
    row_float = (row_start + jnp.arange(slab_rows, dtype=jnp.int32)).astype(jnp.float32)
    col_float = (col_block * tile_len + jnp.arange(tile_len, dtype=jnp.int32)).astype(jnp.float32)
    slab_mask = lax.dynamic_slice_in_dim(mask_float, row_start, slab_rows)
    weighting = (
        (1.0 + (row_float[:, None] + col_float[None, :]) / total_len)
        * slab_mask[:, None]
        * col_mask[None, :]
    )
    update_float = update.astype(jnp.float32)
    partial_sum = jnp.sum(update_float * update_float * weighting[None])
    energy = lax.psum(partial_sum, ("gx", "gy", "gz")) / (total_len * total_len * channel_count)
    return (update, energy)


def solution(mesh):
    in_specs = (P("gx", "gy", None), P(), P(), P(None, None, "gz"), P(), P(), P())
    out_specs = (P(None, ("gx", "gz"), "gy"), P())
    return jax.shard_map(local, mesh=mesh, in_specs=in_specs, out_specs=out_specs, check_vma=False)
```

```python
import jax
import jax.numpy as jnp
from jax import lax
from jax.sharding import PartitionSpec as P

NORM_EPS = 1e-05


def layer_norm(values, gain_vec, axis):
    mean_val = jnp.mean(values, axis=axis, keepdims=True)
    centred = values - mean_val
    variance = jnp.mean(centred * centred, axis=axis, keepdims=True)
    return centred * lax.rsqrt(variance + NORM_EPS) * gain_vec


def batched(first, second):
    return jnp.einsum("hik,hkj->hij", first, second, preferred_element_type=jnp.float32)


def local(pair, residue_mask, ln_in_gain, w_proj, w_gate, ln_out_gain, w_out):
    tile_len = pair.shape[0]
    channel_count = pair.shape[2]
    grid_len = lax.axis_size("gx")
    slab_count = lax.axis_size("gz")
    slab_rows = tile_len // slab_count
    total_len = tile_len * grid_len
    row_block = lax.axis_index("gx")
    col_block = lax.axis_index("gy")
    slab_index = lax.axis_index("gz")
    mask_float = residue_mask.astype(jnp.float32)
    row_mask = lax.dynamic_slice_in_dim(mask_float, row_block * tile_len, tile_len)
    col_mask = lax.dynamic_slice_in_dim(mask_float, col_block * tile_len, tile_len)
    tile_mask = row_mask[:, None] * col_mask[None, :]
    normed = layer_norm(pair.astype(jnp.float32), ln_in_gain, -1).astype(jnp.bfloat16)
    col_len = pair.shape[1]
    col_count = lax.axis_size("gy")
    hidden_here = w_proj.shape[2]
    own_count = hidden_here // (grid_len * col_count)
    piece_count = 2 if own_count % 2 == 0 else 1
    part = own_count // piece_count
    w_parts = w_proj.reshape(channel_count, 4, grid_len * col_count, piece_count, part)

    def operand(weights):
        projected = jnp.einsum("ijd,dkh->khij", normed, weights, preferred_element_type=jnp.float32)
        tile = (tile_mask * jax.nn.sigmoid(projected[0]) * projected[1]).astype(jnp.bfloat16)
        spread = lax.all_to_all(tile, ("gx", "gy"), split_axis=0, concat_axis=0, tiled=True)
        spread = spread.reshape(grid_len, col_count, part, tile_len, col_len)
        return spread.transpose(2, 0, 3, 1, 4).reshape(part, total_len, total_len)

    pieces = []
    for piece in range(piece_count):
        weights = w_parts[:, :, :, piece].reshape(channel_count, 4, -1)
        left = operand(weights[:, :2])
        right = operand(weights[:, 2:])
        summed = batched(left, right) + batched(right, left)
        tri_map = (0.5 * summed).astype(jnp.bfloat16)
        outgoing = tri_map.reshape(part, grid_len, slab_count, slab_rows, col_count, col_len)
        outgoing = outgoing.transpose(1, 4, 2, 0, 3, 5).reshape(-1, slab_rows, col_len)
        pieces.append(
            lax.all_to_all(outgoing, ("gx", "gy", "gz"), split_axis=0, concat_axis=0, tiled=True)
        )
    arrived = jnp.concatenate(pieces, axis=0)

    def by_arrival(table):
        dims = (slab_count, grid_len, col_count, piece_count, part)
        parts = table.reshape(dims + table.shape[1:])
        return jnp.moveaxis(parts, (3, 1, 2), (0, 1, 2)).reshape(table.shape)

    ln_out_gain = by_arrival(ln_out_gain)
    w_out = by_arrival(w_out)
    tri_normed = layer_norm(arrived.astype(jnp.float32), ln_out_gain[:, None, None], 0).astype(jnp.bfloat16)
    mixed = jnp.einsum("hij,hc->cij", tri_normed, w_out, preferred_element_type=jnp.float32)
    slab_normed = lax.dynamic_slice_in_dim(normed, slab_index * slab_rows, slab_rows, 0)
    gate_vals = jax.nn.sigmoid(
        jnp.einsum("ijd,dc->cij", slab_normed, w_gate, preferred_element_type=jnp.float32)
    )
    update = (gate_vals * mixed).astype(jnp.bfloat16)
    row_start = row_block * tile_len + slab_index * slab_rows
    row_float = (row_start + jnp.arange(slab_rows, dtype=jnp.int32)).astype(jnp.float32)
    col_float = (col_block * tile_len + jnp.arange(tile_len, dtype=jnp.int32)).astype(jnp.float32)
    slab_mask = lax.dynamic_slice_in_dim(mask_float, row_start, slab_rows)
    weighting = (
        (1.0 + (row_float[:, None] + col_float[None, :]) / total_len)
        * slab_mask[:, None]
        * col_mask[None, :]
    )
    update_float = update.astype(jnp.float32)
    partial_sum = jnp.sum(update_float * update_float * weighting[None])
    energy = lax.psum(partial_sum, ("gx", "gy", "gz")) / (total_len * total_len * channel_count)
    return (update, energy)


def solution(mesh):
    in_specs = (P("gx", "gy", None), P(), P(), P(None, None, "gz"), P(), P(), P())
    out_specs = (P(None, ("gx", "gz"), "gy"), P())
    return jax.shard_map(local, mesh=mesh, in_specs=in_specs, out_specs=out_specs, check_vma=False)
```
